128 devices in a mesh: rows: 16 (over z, y), cols: 8 (over x, core).
Axes of the slice: x: 4, y: 4, z: 4, core: 2. Of those that a mesh axis runs over, the one named last changes fastest.
Arguments:
- train_query: bfloat16 [8192, 8192], P('rows', 'cols'), may hold values from -0.0625 to 0.0625
- low_query: bfloat16 [8192, 64], P('rows'), may hold values from -0.0625 to 0.0625
- high_query: bfloat16 [64, 8192], P(None, 'cols'), may hold values from -0.75 to 0.75
- train_key: bfloat16 [8192, 512], P('rows', 'cols'), may hold values from -0.0625 to 0.0625
- low_key: bfloat16 [8192, 64], P('rows'), may hold values from -0.0625 to 0.0625
- high_key: bfloat16 [64, 512], P(None, 'cols'), may hold values from -0.75 to 0.75
- train_value: bfloat16 [8192, 512], P('rows', 'cols'), may hold values from -0.0625 to 0.0625
- low_value: bfloat16 [8192, 64], P('rows'), may hold values from -0.0625 to 0.0625
- high_value: bfloat16 [64, 512], P(None, 'cols'), may hold values from -0.75 to 0.75
- norm_train: float32 [8192], P(('rows', 'cols')), may hold values from 0.25 to 1.75
- norm_step: float32 [8192], P(('rows', 'cols')), may hold values from -0.3 to 0.3
Outputs:
- serving_query: bfloat16 [8192, 8192], P('cols')
- serving_key: bfloat16 [512, 8192], P('cols')
- serving_value: bfloat16 [512, 8192], P('cols')
- serve_norm: bfloat16 [8192], replicated
The draws below stay inside these ranges and needn't reach their ends.
All inputs are finite; a program needn't handle non-finite values.
Results may differ from the reference program's by a relative error of at most 0.001.
Values may be sent and summed in bfloat16 or wider, within the bound.
No kernel may reach another device: no remote copies, remote signals or barrier semaphores. Data moves between devices by JAX's collectives and lax.ppermute only.
A program may use at most 128 MiB of HBM per device.

```python
import jax
import jax.numpy as jnp

D_MODEL = 8192
Q_DIM = 8192
KV_DIM = 512
RANK = 64


def steps_of(own_key, extent, cuts, smallest, high):
    def one(dim, shards_of):
        draws = jax.random.uniform(jax.random.fold_in(jax.random.fold_in(own_key, 6), dim), (shards_of,), jnp.float32, smallest / len(cuts), high / len(cuts))
        return jnp.repeat(jnp.exp(draws), extent[dim] // shards_of).reshape((-1,) + (1,) * (len(extent) - dim - 1))

    level = one(*cuts[0])
    for cut in cuts[1:]:
        level = level * one(*cut)
    return level


def normal_values(rng, extent, scale, limit, split=(), kind=jnp.bfloat16):
    gain = steps_of(rng, extent, split, -0.22, 0.18) if split else 1.0
    values = jax.random.normal(rng, extent, jnp.float32) * scale * gain
    return jnp.minimum(jnp.maximum(values, -limit), limit).astype(kind)


def setup_inputs(seed: int = 0) -> dict:
    splits = jax.random.split(jax.random.key(seed), 12)
    return {
        "train_query": normal_values(splits[0], (D_MODEL, Q_DIM), D_MODEL ** -0.5, 0.0625, ((0, 16), (1, 8))),
        "low_query": normal_values(splits[1], (D_MODEL, RANK), D_MODEL ** -0.5, 0.0625, ((0, 16),)),
        "high_query": normal_values(splits[2], (RANK, Q_DIM), RANK ** -0.5, 0.75, ((1, 8),)),
        "train_key": normal_values(splits[3], (D_MODEL, KV_DIM), D_MODEL ** -0.5, 0.0625, ((0, 16), (1, 8))),
        "low_key": normal_values(splits[4], (D_MODEL, RANK), D_MODEL ** -0.5, 0.0625, ((0, 16),)),
        "high_key": normal_values(splits[5], (RANK, KV_DIM), RANK ** -0.5, 0.75, ((1, 8),)),
        "train_value": normal_values(splits[6], (D_MODEL, KV_DIM), D_MODEL ** -0.5, 0.0625, ((0, 16), (1, 8))),
        "low_value": normal_values(splits[7], (D_MODEL, RANK), D_MODEL ** -0.5, 0.0625, ((0, 16),)),
        "high_value": normal_values(splits[8], (RANK, KV_DIM), RANK ** -0.5, 0.75, ((1, 8),)),
        "norm_train": jnp.clip(1.0 + 0.15 * jax.random.normal(splits[9], (D_MODEL,), jnp.float32), 0.25, 1.75),
        "norm_step": jnp.clip(jax.random.uniform(splits[10], (D_MODEL,), jnp.float32, -0.3, 0.3) * steps_of(splits[10], (D_MODEL,), ((0, 128),), -0.4, 0.0), -0.3, 0.3),
    }


mix_rate = 1.0


def reference(train_query, low_query, high_query, train_key, low_key, high_key, train_value, low_value, high_value, norm_train, norm_step):
    whole_query = train_query.astype(jnp.float32) + mix_rate * jnp.dot(low_query, high_query, preferred_element_type=jnp.float32)
    whole_key = train_key.astype(jnp.float32) + mix_rate * jnp.dot(low_key, high_key, preferred_element_type=jnp.float32)
    whole_value = train_value.astype(jnp.float32) + mix_rate * jnp.dot(low_value, high_value, preferred_element_type=jnp.float32)
    serving_query = whole_query.T.astype(jnp.bfloat16)
    serving_key = whole_key.T.astype(jnp.bfloat16)
    serving_value = whole_value.T.astype(jnp.bfloat16)
    serve_norm = (norm_train + norm_step).astype(jnp.bfloat16)
    return serving_query, serving_key, serving_value, serve_norm
```

```python
import functools
import jax
import jax.numpy as jnp
from jax import lax
from jax.experimental import pallas as pl
from jax.experimental.pallas import tpu as pltpu
from jax.sharding import PartitionSpec as P


mix_rate = 1.0


SIDE = 4
CORES = 2
STEP = 128
CHUNK = 256
MERGE_VMEM = 65_860_000
PARTS = 2


def merge_kernel(*refs):
    out, held, sem = refs[9], refs[10:-1], refs[-1]
    train, low, high, key, low_key, high_key, value, low_value, high_value = held
    rows, wide = train.shape
    parts = [pl.ds(at, STEP) for at in range(0, rows, STEP)]
    rest = len(parts)
    copies = [pltpu.make_async_copy(refs[0].at[part], train.at[part], sem.at[i]) for i, part in enumerate(parts)]
    copies += [pltpu.make_async_copy(refs[i], held[i], sem.at[rest + i - 1]) for i in range(1, 9)]
    order = [rest, rest + 1, *range(rest), *range(rest + 2, rest + 8)]
    for i in order:
        copies[i].start()

    def product(left, right):
        return lax.dot_general(right, left, (((0,), (0,)), ((), ())), preferred_element_type=jnp.float32)

    copies[rest].wait()
    copies[rest + 1].wait()
    for copy, part in zip(copies, parts):
        copy.wait()
        for at in range(0, wide, CHUNK):
            base = train[part, at : at + CHUNK].T.astype(jnp.float32)
            whole = base + mix_rate * product(low[:, part], high[:, at : at + CHUNK])
            out[at : at + CHUNK, part] = whole.astype(jnp.bfloat16)
    for copy in copies[rest + 2 :]:
        copy.wait()
    at = wide
    for base, left, right in ((key, low_key, high_key), (value, low_value, high_value)):
        whole = base[...].astype(jnp.float32) + mix_rate * product(left[...], right[...])
        out[at : at + base.shape[0], :] = whole.astype(jnp.bfloat16)
        at += base.shape[0]


def merged(train, low, high, train_key, low_key, high_key, train_value, low_value, high_value):
    rows, columns = train.shape
    total = columns + train_key.shape[1] + train_value.shape[1]
    small = (low.T, high, train_key.T, low_key.T, high_key, train_value.T, low_value.T, high_value)
    return pl.pallas_call(
        merge_kernel,
        in_specs=[pl.BlockSpec(memory_space=pltpu.HBM)] * 9,
        out_specs=pl.BlockSpec(memory_space=pltpu.VMEM),
        out_shape=jax.ShapeDtypeStruct((total, rows), jnp.bfloat16),
        scratch_shapes=[
            pltpu.VMEM(train.shape, train.dtype),
            *[pltpu.VMEM(x.shape, x.dtype) for x in small],
            pltpu.SemaphoreType.DMA((8 + rows // STEP,)),
        ],
        compiler_params=pltpu.CompilerParams(vmem_limit_bytes=MERGE_VMEM),
        cost_estimate=pl.CostEstimate(flops=10**8, bytes_accessed=10**7, transcendentals=0),
        name="merge",
    )(train, *small)


def place_kernel(plan, *refs):
    count = len(plan)
    pieces = refs[:count]
    outs, held, into, out_of = refs[-count - 5 : -count - 2], refs[-count - 2 : -2], refs[-2], refs[-1]
    rank = lax.axis_index("rows")
    first_axis_is_y = lax.rem(lax.axis_index("cols"), CORES) == 0
    y, z = lax.rem(rank, SIDE), lax.div(rank, SIDE)
    reads, writes = [], []
    for piece, kept, (first, one, two) in zip(pieces, held, plan):
        dy, dz = jnp.where(first_axis_is_y, one, two), jnp.where(first_axis_is_y, two, one)
        origin = lax.rem(z + dz, SIDE) * SIDE + lax.rem(y + dy, SIDE)
        width = piece.shape[1]
        at = pl.ds(pl.multiple_of(origin * width, width), width)
        half = piece.shape[0] // PARTS
        for part in range(PARTS):
            low, high = part * half, (part + 1) * half
            reads.append(
                pltpu.make_async_copy(piece.at[pl.ds(low, half)], kept.at[pl.ds(low, half)], into.at[len(reads)])
            )
            group, start = [], 0
            for out in outs:
                stop = start + out.shape[0]
                begin, end = max(start, first + low), min(stop, first + high)
                if begin < end:
                    group.append((kept.at[pl.ds(begin - first, end - begin)], out.at[pl.ds(begin - start, end - begin), at]))
                start = stop
            writes.append(group)
    for read in reads:
        read.start()
    started = []
    for read, group in zip(reads, writes):
        read.wait()
        for source, target in group:
            started.append(pltpu.make_async_copy(source, target, out_of.at[len(started)]))
            started[-1].start()
    for copy in started:
        copy.wait()


def place(pieces, plan, outs, shapes):
    count = len(pieces)
    hbm = pl.BlockSpec(memory_space=pltpu.HBM)
    given = () if outs is None else outs
    return pl.pallas_call(
        functools.partial(place_kernel, tuple(plan)),
        in_specs=[hbm] * (count + len(given)),
        out_specs=[hbm] * 3,
        out_shape=shapes,
        scratch_shapes=[
            *[pltpu.VMEM(p.shape, p.dtype) for p in pieces],
            pltpu.SemaphoreType.DMA((PARTS * count,)),
            pltpu.SemaphoreType.DMA((PARTS * count + 3 * count,)),
        ],
        input_output_aliases={count + i: i for i in range(len(given))},
        compiler_params=pltpu.CompilerParams(vmem_limit_bytes=5 << 20),
        cost_estimate=pl.CostEstimate(
            flops=10**6, bytes_accessed=4 * sum(p.size for p in pieces), transcendentals=0
        ),
        name="place",
    )(*pieces, *given)


def along(second, by):
    pairs = []
    for z in range(SIDE):
        for y in range(SIDE):
            for x in range(SIDE):
                for core in range(CORES):
                    on_z = (core == 1) != second
                    to_z, to_y = ((z + by) % SIDE, y) if on_z else (z, (y + by) % SIDE)
                    flat = lambda r, q: ((r * SIDE + q) * SIDE + x) * CORES + core
                    pairs.append((flat(z, y), flat(to_z, to_y)))
    return pairs


def exchange(mine, bit, swapped):
    count = SIDE * SIDE * SIDE * CORES
    pick = lambda i: swapped if i % CORES else bit
    other = lax.ppermute(mine, ("rows", "cols"), [(i, i ^ pick(i)) for i in range(count)])
    index = lax.axis_index(("rows", "cols"))
    mask = jnp.where(index % CORES == 0, bit, swapped)
    return jnp.where((index & mask) == 0, jnp.concatenate([mine, other]), jnp.concatenate([other, mine]))


def in_order(norm):
    four = norm.reshape(SIDE, SIDE, SIDE, -1)
    on_y = lax.axis_index("cols") % CORES == 0
    return jnp.where(on_y, four.transpose(2, 0, 1, 3), four.transpose(0, 2, 1, 3)).reshape(-1)


def body(
    train_query,
    low_query,
    high_query,
    train_key,
    low_key,
    high_key,
    train_value,
    low_value,
    high_value,
    norm_train,
    norm_step,
):
    shapes = [
        jax.ShapeDtypeStruct((w.shape[1], w.shape[0] * SIDE * SIDE), jnp.bfloat16)
        for w in (train_query, train_key, train_value)
    ]
    own = merged(train_query, low_query, high_query, train_key, low_key, high_key, train_value, low_value, high_value)
    part = own.shape[0] // 2

    def one(x, by):
        return lax.ppermute(x, ("rows", "cols"), along(False, by))

    def two(x, by):
        return lax.ppermute(x, ("rows", "cols"), along(True, by))

    outs = None

    def put(pieces, plan):
        nonlocal outs
        outs = place(pieces, plan, outs, shapes)

    a_up, a_down = one(own, 1), one(own, -1)
    norm = (norm_train + norm_step).astype(jnp.bfloat16)
    norm = exchange(norm, 1, 1)
    norm = exchange(norm, 32, 8)
    norm = exchange(norm, 64, 16)
    c_up, c_down = two(own, 1), two(own, -1)
    norm = exchange(norm, 2, 2)
    put([own], [(0, 0, 0)])
    norm = exchange(norm, 4, 4)
    b = one(a_up, 1)
    d_down = two(a_up, -1)
    g_down = two(a_down, -1)
    put([a_up, a_down], [(0, 3, 0), (0, 1, 0)])
    far = two(c_up, 1)
    put([c_up, c_down], [(0, 0, 3), (0, 0, 1)])
    d_up = two(a_up, 1)
    g_up = two(a_down, 1)
    norm = exchange(norm, 8, 32)
    e_down, e_up = two(b, -1), two(b, 1)
    g_far = two(g_down, -1)
    put([b, d_down], [(0, 2, 0), (0, 3, 1)])
    norm = exchange(norm, 16, 64)
    d_far_low = two(d_down[part:], -1)
    e_far = two(e_down, -1)
    put([far, g_down], [(0, 0, 2), (0, 1, 1)])
    d_far_top = two(d_up[:part], 1)
    put([d_up, e_down], [(0, 3, 3), (0, 2, 1)])
    serve_norm = in_order(norm)
    put([g_up, g_far], [(0, 1, 3), (0, 1, 2)])
    put([e_up, e_far], [(0, 2, 3), (0, 2, 2)])
    put([d_far_top, d_far_low], [(0, 3, 2), (part, 3, 2)])
    return (*outs, serve_norm)


def solution(mesh):
    return jax.shard_map(
        body,
        mesh=mesh,
        in_specs=(
            P("rows", "cols"),
            P("rows", None),
            P(None, "cols"),
            P("rows", "cols"),
            P("rows", None),
            P(None, "cols"),
            P("rows", "cols"),
            P("rows", None),
            P(None, "cols"),
            P(("rows", "cols")),
            P(("rows", "cols")),
        ),
        out_specs=(P("cols", None), P("cols", None), P("cols", None), P()),
        check_vma=False,
    )
```

```python
import functools
import jax
import jax.numpy as jnp
from jax import lax
from jax.experimental import pallas as pl
from jax.experimental.pallas import tpu as pltpu
from jax.sharding import PartitionSpec as P


mix_rate = 1.0


SIDE = 4
CORES = 2
STEP = 128
CHUNK = 256
MERGE_VMEM = 65_000_000
PARTS = 2


def product(left, right):
    return lax.dot_general(right, left, (((0,), (0,)), ((), ())), preferred_element_type=jnp.float32)


def fill(train_copies, parts, train, low, high, out):
    for copy, part in zip(train_copies, parts):
        copy.wait()
        for at in range(0, train.shape[1], CHUNK):
            base = train[part, at : at + CHUNK].T.astype(jnp.float32)
            whole = base + mix_rate * product(low[:, part], high[:, at : at + CHUNK])
            out[at : at + CHUNK, part] = whole.astype(jnp.bfloat16)


def merge_kernel(*refs):
    out, side, held, sem = refs[9], refs[10], refs[11:-1], refs[-1]
    train, low, high, key, low_key, high_key, value, low_value, high_value = held
    rows, wide = train.shape
    parts = [pl.ds(at, STEP) for at in range(0, rows, STEP)]
    rest = len(parts)
    copies = [pltpu.make_async_copy(refs[0].at[part], train.at[part], sem.at[i]) for i, part in enumerate(parts)]
    copies += [pltpu.make_async_copy(refs[i], held[i], sem.at[rest + i - 1]) for i in range(1, 9)]
    order = [rest, rest + 1, *range(rest), *range(rest + 2, rest + 8)]
    for i in order:
        copies[i].start()
    copies[rest].wait()
    copies[rest + 1].wait()
    fill(copies, parts, train, low, high, out)
    for copy in copies[rest + 2 :]:
        copy.wait()
    at = wide
    for base, left, right in ((key, low_key, high_key), (value, low_value, high_value)):
        whole = base[...].astype(jnp.float32) + mix_rate * product(left[...], right[...])
        whole = whole.astype(jnp.bfloat16)
        out[at : at + base.shape[0], :] = whole
        side[at - wide : at - wide + base.shape[0], :] = whole
        at += base.shape[0]
    side[at - wide :, :] = low[...]


def merged(train, low, high, train_key, low_key, high_key, train_value, low_value, high_value):
    rows, columns = train.shape
    extra = train_key.shape[1] + train_value.shape[1]
    small = (low.T, high, train_key.T, low_key.T, high_key, train_value.T, low_value.T, high_value)
    return pl.pallas_call(
        merge_kernel,
        in_specs=[pl.BlockSpec(memory_space=pltpu.HBM)] * 9,
        out_specs=[pl.BlockSpec(memory_space=pltpu.VMEM)] * 2,
        out_shape=[
            jax.ShapeDtypeStruct((columns + extra, rows), jnp.bfloat16),
            jax.ShapeDtypeStruct((extra + low.shape[1], rows), jnp.bfloat16),
        ],
        scratch_shapes=[
            pltpu.VMEM(train.shape, train.dtype),
            *[pltpu.VMEM(x.shape, x.dtype) for x in small],
            pltpu.SemaphoreType.DMA((8 + rows // STEP,)),
        ],
        compiler_params=pltpu.CompilerParams(vmem_limit_bytes=MERGE_VMEM),
        cost_estimate=pl.CostEstimate(flops=10**9, bytes_accessed=1, transcendentals=0),
        name="merge",
    )(train, *small)


def finish_kernel(train_ref, side_ref, high_ref, out, train, side, high, sem):
    rows, wide = train.shape
    extra = out.shape[0] - wide
    parts = [pl.ds(at, STEP) for at in range(0, rows, STEP)]
    rest = len(parts)
    copies = [pltpu.make_async_copy(train_ref.at[part], train.at[part], sem.at[i]) for i, part in enumerate(parts)]
    copies.append(pltpu.make_async_copy(side_ref, side, sem.at[rest]))
    copies.append(pltpu.make_async_copy(high_ref, high, sem.at[rest + 1]))
    for copy in copies[rest:] + copies[:rest]:
        copy.start()
    copies[rest].wait()
    copies[rest + 1].wait()
    out[wide:, :] = side[:extra, :]
    fill(copies, parts, train, side.at[pl.ds(extra, side.shape[0] - extra)], high, out)


def finished(train, side, high):
    rows, wide = train.shape
    extra = side.shape[0] - high.shape[0]
    return pl.pallas_call(
        finish_kernel,
        in_specs=[pl.BlockSpec(memory_space=pl.ANY)] * 3,
        out_specs=pl.BlockSpec(memory_space=pltpu.VMEM),
        out_shape=jax.ShapeDtypeStruct((wide + extra, rows), jnp.bfloat16),
        scratch_shapes=[
            *[pltpu.VMEM(x.shape, x.dtype) for x in (train, side, high)],
            pltpu.SemaphoreType.DMA((2 + rows // STEP,)),
        ],
        compiler_params=pltpu.CompilerParams(vmem_limit_bytes=8 << 20),
        cost_estimate=pl.CostEstimate(flops=10**9, bytes_accessed=1, transcendentals=0),
        name="finish",
    )(train, side, high)


def place_kernel(plan, direct, *refs):
    count = len(plan)
    pieces = refs[:count]
    outs, held, into, out_of = refs[-count - 5 : -count - 2], refs[-count - 2 : -2], refs[-2], refs[-1]
    rank = lax.axis_index("rows")
    first_axis_is_y = lax.rem(lax.axis_index("cols"), CORES) == 0
    y, z = lax.rem(rank, SIDE), lax.div(rank, SIDE)
    reads, writes = [], []
    for piece, kept, straight, (first, one, two) in zip(pieces, held, direct, plan):
        dy, dz = jnp.where(first_axis_is_y, one, two), jnp.where(first_axis_is_y, two, one)
        origin = lax.rem(z + dz, SIDE) * SIDE + lax.rem(y + dy, SIDE)
        width = piece.shape[1]
        at = pl.ds(pl.multiple_of(origin * width, width), width)
        half = piece.shape[0] // PARTS
        for part in range(PARTS):
            low, high = part * half, (part + 1) * half
            if straight:
                kept = piece
                reads.append(None)
            else:
                reads.append(
                    pltpu.make_async_copy(piece.at[pl.ds(low, half)], kept.at[pl.ds(low, half)], into.at[len(reads)])
                )
            group, start = [], 0
            for out in outs:
                stop = start + out.shape[0]
                begin, end = max(start, first + low), min(stop, first + high)
                if begin < end:
                    group.append((kept.at[pl.ds(begin - first, end - begin)], out.at[pl.ds(begin - start, end - begin), at]))
                start = stop
            writes.append(group)
    for read in reads:
        if read is not None:
            read.start()
    started = []
    for read, group in sorted(zip(reads, writes), key=lambda both: both[0] is not None):
        if read is not None:
            read.wait()
        for source, target in group:
            started.append(pltpu.make_async_copy(source, target, out_of.at[len(started)]))
            started[-1].start()
    for copy in started:
        copy.wait()


def place(pieces, plan, outs, shapes, direct):
    count = len(pieces)
    hbm = pl.BlockSpec(memory_space=pltpu.HBM)
    given = () if outs is None else outs
    return pl.pallas_call(
        functools.partial(place_kernel, tuple(plan), direct),
        in_specs=[pl.BlockSpec(memory_space=pl.ANY)] * count + [hbm] * len(given),
        out_specs=[hbm] * 3,
        out_shape=shapes,
        scratch_shapes=[
            *[pltpu.VMEM((16, 128) if straight else p.shape, p.dtype) for p, straight in zip(pieces, direct)],
            pltpu.SemaphoreType.DMA((PARTS * count,)),
            pltpu.SemaphoreType.DMA((PARTS * count + 3 * count,)),
        ],
        input_output_aliases={count + i: i for i in range(len(given))},
        compiler_params=pltpu.CompilerParams(vmem_limit_bytes=5 << 20),
        cost_estimate=pl.CostEstimate(
            flops=10**6, bytes_accessed=4 * sum(p.size for p in pieces), transcendentals=0
        ),
        name="place",
    )(*pieces, *given)


def along(second, by):
    pairs = []
    for z in range(SIDE):
        for y in range(SIDE):
            for x in range(SIDE):
                for core in range(CORES):
                    on_z = (core == 1) != second
                    to_z, to_y = ((z + by) % SIDE, y) if on_z else (z, (y + by) % SIDE)
                    flat = lambda r, q: ((r * SIDE + q) * SIDE + x) * CORES + core
                    pairs.append((flat(z, y), flat(to_z, to_y)))
    return pairs


def join_kernel(mine_ref, other_ref, out_ref):
    rows, width = mine_ref.shape
    out_ref[:rows, :width] = mine_ref[...]
    if out_ref.shape[0] > rows:
        out_ref[rows:, :] = other_ref[...]
    else:
        out_ref[:, width:] = other_ref[...]


def joined(mine, other, wider):
    rows, width = mine.shape
    vmem = pl.BlockSpec(memory_space=pltpu.VMEM)
    return pl.pallas_call(
        join_kernel,
        in_specs=[vmem] * 2,
        out_specs=vmem,
        out_shape=jax.ShapeDtypeStruct((rows, 2 * width) if wider else (2 * rows, width), mine.dtype),
        compiler_params=pltpu.CompilerParams(vmem_limit_bytes=1 << 20),
        name="join",
    )(mine, other)


def exchange(mine, bit, swapped):
    count = SIDE * SIDE * SIDE * CORES
    pick = lambda i: swapped if i % CORES else bit
    other = lax.ppermute(mine, ("rows", "cols"), [(i, i ^ pick(i)) for i in range(count)])
    return joined(mine, other, bit == 1)


def order_kernel(norm_ref, out_ref, rows, held):
    cell, rank = lax.axis_index("cols"), lax.axis_index("rows")
    core, x = lax.rem(cell, CORES), lax.div(cell, CORES)
    y, z = lax.rem(rank, SIDE), lax.div(rank, SIDE)
    side = norm_ref.shape[1] // 2
    rolled = pltpu.roll(norm_ref[...], side, 1)
    held[...] = jnp.where(core == 0, norm_ref[...], rolled)
    for i in range(SIDE * SIDE * SIDE):
        dz, dy, dx = (i // 16) ^ z, (i // 4 % 4) ^ y, (i % 4) ^ x
        row = jnp.where(core == 0, dy * 16 + dx * 4 + dz, dz * 16 + dx * 4 + dy)
        rows[pl.ds(i, 1), :] = held[pl.ds(row, 1), :]
    out_ref[...] = rows[...].astype(jnp.bfloat16)


def in_order(norm):
    vmem = pl.BlockSpec(memory_space=pltpu.VMEM)
    return pl.pallas_call(
        order_kernel,
        in_specs=[vmem],
        out_specs=vmem,
        out_shape=jax.ShapeDtypeStruct(norm.shape, jnp.bfloat16),
        scratch_shapes=[pltpu.VMEM(norm.shape, norm.dtype)] * 2,
        compiler_params=pltpu.CompilerParams(vmem_limit_bytes=1 << 20),
        name="order",
    )(norm).reshape(-1)


def body(
    train_query,
    low_query,
    high_query,
    train_key,
    low_key,
    high_key,
    train_value,
    low_value,
    high_value,
    norm_train,
    norm_step,
):
    shapes = [
        jax.ShapeDtypeStruct((w.shape[1], w.shape[0] * SIDE * SIDE), jnp.bfloat16)
        for w in (train_query, train_key, train_value)
    ]
    own, side = merged(
        train_query, low_query, high_query, train_key, low_key, high_key, train_value, low_value, high_value
    )
    part = own.shape[0] * 13 // 24

    def one(x, by):
        return lax.ppermute(x, ("rows", "cols"), along(False, by))

    def two(x, by):
        return lax.ppermute(x, ("rows", "cols"), along(True, by))

    outs = None

    def put(name, pieces, plan, direct=()):
        nonlocal outs
        direct = (name != "put_own",) * len(pieces)
        outs = place(pieces, plan, outs, shapes, direct)

    raw_up, raw_down = one(train_query, 1), one(train_query, -1)
    side_up, side_down = one(side, 1), one(side, -1)
    a_up = finished(raw_up, side_up, high_query)
    a_down = finished(raw_down, side_down, high_query)
    norm = (norm_train + norm_step).reshape(1, -1)
    norm = exchange(norm, 1, 1)
    norm = exchange(norm, 32, 8)
    norm = exchange(norm, 64, 16)
    c_up, c_down = two(own, 1), two(own, -1)
    b = one(a_up, 1)
    d_down, d_up = two(a_up, -1), two(a_up, 1)
    g_down, g_up = two(a_down, -1), two(a_down, 1)
    far = two(c_down, -1)
    put("put_own", [own], [(0, 0, 0)])
    put("put_c", [c_up, c_down], [(0, 0, 3), (0, 0, 1)])
    put("put_a", [a_up, a_down], [(0, 3, 0), (0, 1, 0)])
    norm = exchange(norm, 2, 2)
    norm = exchange(norm, 4, 4)
    e_down, e_up = two(b, -1), two(b, 1)
    put("put_b", [b, d_down], [(0, 2, 0), (0, 3, 1)])
    norm = exchange(norm, 8, 32)
    d_far_low = two(d_down[part:], -1)
    put("put_d", [d_up, g_down], [(0, 3, 3), (0, 1, 1)])
    norm = exchange(norm, 16, 64)
    g_far = two(g_up, 1)
    d_far_top = two(d_up[:part], 1)
    put("put_g", [g_up, far], [(0, 1, 3), (0, 0, 2)])
    e_far = two(e_down, -1)
    put("put_e", [e_up, e_down], [(0, 2, 3), (0, 2, 1)])
    serve_norm = in_order(norm)
    put("put_f", [g_far, d_far_low], [(0, 1, 2), (part, 3, 2)])
    put("put_h", [e_far, d_far_top], [(0, 2, 2), (0, 3, 2)])
    return (*outs, serve_norm)


def solution(mesh):
    return jax.shard_map(
        body,
        mesh=mesh,
        in_specs=(
            P("rows", "cols"),
            P("rows", None),
            P(None, "cols"),
            P("rows", "cols"),
            P("rows", None),
            P(None, "cols"),
            P("rows", "cols"),
            P("rows", None),
            P(None, "cols"),
            P(("rows", "cols")),
            P(("rows", "cols")),
        ),
        out_specs=(P("cols", None), P("cols", None), P("cols", None), P()),
        check_vma=False,
    )
```

```python
import functools
import jax
import jax.numpy as jnp
from jax import lax
from jax.experimental import pallas as pl
from jax.experimental.pallas import tpu as pltpu
from jax.sharding import PartitionSpec as P


mix_rate = 1.0


SIDE = 4
CORES = 2
STEP = 128
CHUNK = 256
MERGE_VMEM = 65_000_000
PARTS = 1


def product(left, right):
    return lax.dot_general(right, left, (((0,), (0,)), ((), ())), preferred_element_type=jnp.float32)


def fill(train_copies, parts, train, low, high, out):
    for copy, part in zip(train_copies, parts):
        copy.wait()
        for at in range(0, train.shape[1], CHUNK):
            base = train[part, at : at + CHUNK].T.astype(jnp.float32)
            whole = base + mix_rate * product(low[:, part], high[:, at : at + CHUNK])
            out[at : at + CHUNK, part] = whole.astype(jnp.bfloat16)


def merge_kernel(*refs):
    out, side, held, sem = refs[9], refs[10], refs[11:-1], refs[-1]
    train, low, high, key, low_key, high_key, value, low_value, high_value = held
    rows, wide = train.shape
    parts = [pl.ds(at, STEP) for at in range(0, rows, STEP)]
    rest = len(parts)
    copies = [pltpu.make_async_copy(refs[0].at[part], train.at[part], sem.at[i]) for i, part in enumerate(parts)]
    copies += [pltpu.make_async_copy(refs[i], held[i], sem.at[rest + i - 1]) for i in range(1, 9)]
    order = [rest, rest + 1, *range(rest), *range(rest + 2, rest + 8)]
    for i in order:
        copies[i].start()
    copies[rest].wait()
    copies[rest + 1].wait()
    fill(copies, parts, train, low, high, out)
    for copy in copies[rest + 2 :]:
        copy.wait()
    at = wide
    for base, left, right in ((key, low_key, high_key), (value, low_value, high_value)):
        whole = base[...].astype(jnp.float32) + mix_rate * product(left[...], right[...])
        whole = whole.astype(jnp.bfloat16)
        out[at : at + base.shape[0], :] = whole
        side[at - wide : at - wide + base.shape[0], :] = whole
        at += base.shape[0]
    side[at - wide :, :] = low[...]


def merged(train, low, high, train_key, low_key, high_key, train_value, low_value, high_value):
    rows, columns = train.shape
    extra = train_key.shape[1] + train_value.shape[1]
    small = (low.T, high, train_key.T, low_key.T, high_key, train_value.T, low_value.T, high_value)
    return pl.pallas_call(
        merge_kernel,
        in_specs=[pl.BlockSpec(memory_space=pltpu.HBM)] * 9,
        out_specs=[pl.BlockSpec(memory_space=pltpu.VMEM)] * 2,
        out_shape=[
            jax.ShapeDtypeStruct((columns + extra, rows), jnp.bfloat16),
            jax.ShapeDtypeStruct((extra + low.shape[1], rows), jnp.bfloat16),
        ],
        scratch_shapes=[
            pltpu.VMEM(train.shape, train.dtype),
            *[pltpu.VMEM(x.shape, x.dtype) for x in small],
            pltpu.SemaphoreType.DMA((8 + rows // STEP,)),
        ],
        compiler_params=pltpu.CompilerParams(vmem_limit_bytes=MERGE_VMEM),
        cost_estimate=pl.CostEstimate(flops=10**9, bytes_accessed=1, transcendentals=0),
        name="merge",
    )(train, *small)


def finish_kernel(train_ref, side_ref, high_ref, out, train, side, high, sem):
    rows, wide = train.shape
    extra = out.shape[0] - wide
    parts = [pl.ds(at, STEP) for at in range(0, rows, STEP)]
    rest = len(parts)
    copies = [pltpu.make_async_copy(train_ref.at[part], train.at[part], sem.at[i]) for i, part in enumerate(parts)]
    copies.append(pltpu.make_async_copy(side_ref, side, sem.at[rest]))
    copies.append(pltpu.make_async_copy(high_ref, high, sem.at[rest + 1]))
    for copy in copies[rest:] + copies[:rest]:
        copy.start()
    copies[rest].wait()
    copies[rest + 1].wait()
    out[wide:, :] = side[:extra, :]
    fill(copies, parts, train, side.at[pl.ds(extra, side.shape[0] - extra)], high, out)


def finished(train, side, high):
    rows, wide = train.shape
    extra = side.shape[0] - high.shape[0]
    return pl.pallas_call(
        finish_kernel,
        in_specs=[pl.BlockSpec(memory_space=pl.ANY)] * 3,
        out_specs=pl.BlockSpec(memory_space=pltpu.VMEM),
        out_shape=jax.ShapeDtypeStruct((wide + extra, rows), jnp.bfloat16),
        scratch_shapes=[
            *[pltpu.VMEM(x.shape, x.dtype) for x in (train, side, high)],
            pltpu.SemaphoreType.DMA((2 + rows // STEP,)),
        ],
        compiler_params=pltpu.CompilerParams(vmem_limit_bytes=8 << 20),
        cost_estimate=pl.CostEstimate(flops=10**9, bytes_accessed=1, transcendentals=0),
        name="finish",
    )(train, side, high)


def place_kernel(plan, direct, *refs):
    count = len(plan)
    pieces = refs[:count]
    outs, held, into, out_of = refs[-count - 5 : -count - 2], refs[-count - 2 : -2], refs[-2], refs[-1]
    rank = lax.axis_index("rows")
    first_axis_is_y = lax.rem(lax.axis_index("cols"), CORES) == 0
    y, z = lax.rem(rank, SIDE), lax.div(rank, SIDE)
    reads, writes = [], []
    for piece, kept, straight, (first, one, two) in zip(pieces, held, direct, plan):
        dy, dz = jnp.where(first_axis_is_y, one, two), jnp.where(first_axis_is_y, two, one)
        origin = lax.rem(z + dz, SIDE) * SIDE + lax.rem(y + dy, SIDE)
        width = piece.shape[1]
        at = pl.ds(pl.multiple_of(origin * width, width), width)
        half = piece.shape[0] // PARTS
        for part in range(PARTS):
            low, high = part * half, (part + 1) * half
            if straight:
                kept = piece
                reads.append(None)
            else:
                reads.append(
                    pltpu.make_async_copy(piece.at[pl.ds(low, half)], kept.at[pl.ds(low, half)], into.at[len(reads)])
                )
            group, start = [], 0
            for out in outs:
                stop = start + out.shape[0]
                begin, end = max(start, first + low), min(stop, first + high)
                if begin < end:
                    group.append((kept.at[pl.ds(begin - first, end - begin)], out.at[pl.ds(begin - start, end - begin), at]))
                start = stop
            writes.append(group)
    for read in reads:
        if read is not None:
            read.start()
    started = []
    for read, group in sorted(zip(reads, writes), key=lambda both: both[0] is not None):
        if read is not None:
            read.wait()
        for source, target in group:
            started.append(pltpu.make_async_copy(source, target, out_of.at[len(started)]))
            started[-1].start()
    for copy in started:
        copy.wait()


def place(pieces, plan, outs, shapes, direct):
    count = len(pieces)
    hbm = pl.BlockSpec(memory_space=pltpu.HBM)
    given = () if outs is None else outs
    return pl.pallas_call(
        functools.partial(place_kernel, tuple(plan), direct),
        in_specs=[pl.BlockSpec(memory_space=pl.ANY)] * count + [hbm] * len(given),
        out_specs=[hbm] * 3,
        out_shape=shapes,
        scratch_shapes=[
            *[pltpu.VMEM((16, 128) if straight else p.shape, p.dtype) for p, straight in zip(pieces, direct)],
            pltpu.SemaphoreType.DMA((PARTS * count,)),
            pltpu.SemaphoreType.DMA((PARTS * count + 3 * count,)),
        ],
        input_output_aliases={count + i: i for i in range(len(given))},
        compiler_params=pltpu.CompilerParams(vmem_limit_bytes=5 << 20),
        cost_estimate=pl.CostEstimate(
            flops=10**6, bytes_accessed=4 * sum(p.size for p in pieces), transcendentals=0
        ),
        name="place",
    )(*pieces, *given)


def along(second, by):
    pairs = []
    for z in range(SIDE):
        for y in range(SIDE):
            for x in range(SIDE):
                for core in range(CORES):
                    on_z = (core == 1) != second
                    to_z, to_y = ((z + by) % SIDE, y) if on_z else (z, (y + by) % SIDE)
                    flat = lambda r, q: ((r * SIDE + q) * SIDE + x) * CORES + core
                    pairs.append((flat(z, y), flat(to_z, to_y)))
    return pairs


def join_kernel(mine_ref, other_ref, out_ref):
    rows, width = mine_ref.shape
    out_ref[:rows, :width] = mine_ref[...]
    if out_ref.shape[0] > rows:
        out_ref[rows:, :] = other_ref[...]
    else:
        out_ref[:, width:] = other_ref[...]


def joined(mine, other, wider):
    rows, width = mine.shape
    vmem = pl.BlockSpec(memory_space=pltpu.VMEM)
    return pl.pallas_call(
        join_kernel,
        in_specs=[vmem] * 2,
        out_specs=vmem,
        out_shape=jax.ShapeDtypeStruct((rows, 2 * width) if wider else (2 * rows, width), mine.dtype),
        compiler_params=pltpu.CompilerParams(vmem_limit_bytes=1 << 20),
        name="join",
    )(mine, other)


def exchange(mine, bit, swapped):
    count = SIDE * SIDE * SIDE * CORES
    pick = lambda i: swapped if i % CORES else bit
    other = lax.ppermute(mine, ("rows", "cols"), [(i, i ^ pick(i)) for i in range(count)])
    return joined(mine, other, bit == 1)


def order_kernel(norm_ref, out_ref, rows, held):
    cell, rank = lax.axis_index("cols"), lax.axis_index("rows")
    core, x = lax.rem(cell, CORES), lax.div(cell, CORES)
    y, z = lax.rem(rank, SIDE), lax.div(rank, SIDE)
    side = norm_ref.shape[1] // 2
    rolled = pltpu.roll(norm_ref[...], side, 1)
    held[...] = jnp.where(core == 0, norm_ref[...], rolled)
    for i in range(SIDE * SIDE * SIDE):
        dz, dy, dx = (i // 16) ^ z, (i // 4 % 4) ^ y, (i % 4) ^ x
        row = jnp.where(core == 0, dy * 16 + dx * 4 + dz, dz * 16 + dx * 4 + dy)
        rows[pl.ds(i, 1), :] = held[pl.ds(row, 1), :]
    out_ref[...] = rows[...].astype(jnp.bfloat16)


def in_order(norm):
    vmem = pl.BlockSpec(memory_space=pltpu.VMEM)
    return pl.pallas_call(
        order_kernel,
        in_specs=[vmem],
        out_specs=vmem,
        out_shape=jax.ShapeDtypeStruct(norm.shape, jnp.bfloat16),
        scratch_shapes=[pltpu.VMEM(norm.shape, norm.dtype)] * 2,
        compiler_params=pltpu.CompilerParams(vmem_limit_bytes=1 << 20),
        name="order",
    )(norm).reshape(-1)


def body(
    train_query,
    low_query,
    high_query,
    train_key,
    low_key,
    high_key,
    train_value,
    low_value,
    high_value,
    norm_train,
    norm_step,
):
    shapes = [
        jax.ShapeDtypeStruct((w.shape[1], w.shape[0] * SIDE * SIDE), jnp.bfloat16)
        for w in (train_query, train_key, train_value)
    ]
    own, side = merged(
        train_query, low_query, high_query, train_key, low_key, high_key, train_value, low_value, high_value
    )
    total = own.shape[0]
    cuts = (total * 5 // 12, total * 19 // 36, train_query.shape[1])

    def one(x, by):
        return lax.ppermute(x, ("rows", "cols"), along(False, by))

    def two(x, by):
        return lax.ppermute(x, ("rows", "cols"), along(True, by))

    outs = None

    def put(name, pieces, plan, direct=()):
        nonlocal outs
        direct = (name != "put_own",) * len(pieces)
        outs = place(pieces, plan, outs, shapes, direct)

    raw_up, raw_down = one(train_query, 1), one(train_query, -1)
    side_up, side_down = one(side, 1), one(side, -1)
    a_up = finished(raw_up, side_up, high_query)
    a_down = finished(raw_down, side_down, high_query)
    norm = (norm_train + norm_step).reshape(1, -1)
    norm = exchange(norm, 1, 1)
    norm = exchange(norm, 32, 8)
    norm = exchange(norm, 64, 16)
    c_up, c_down = two(own, 1), two(own, -1)
    b = one(a_up, 1)
    d_down, d_up = two(a_up, -1), two(a_up, 1)
    g_down, g_up = two(a_down, -1), two(a_down, 1)
    far = two(c_down, -1)
    put("put_own", [own], [(0, 0, 0)])
    put("put_c", [c_up, c_down], [(0, 0, 3), (0, 0, 1)])
    put("put_a", [a_up, a_down], [(0, 3, 0), (0, 1, 0)])
    norm = exchange(norm, 2, 2)
    low1 = two(d_down[cuts[1] : cuts[2]], -1)
    low2 = two(d_down[cuts[2] :], -1)
    e_down, e_up = two(b, -1), two(b, 1)
    put("put_b", [b, d_down], [(0, 2, 0), (0, 3, 1)])
    norm = exchange(norm, 4, 4)
    put("put_d", [d_up, g_down], [(0, 3, 3), (0, 1, 1)])
    norm = exchange(norm, 8, 32)
    g_far = two(g_up, 1)
    top1 = two(d_up[: cuts[0]], 1)
    top2 = two(d_up[cuts[0] : cuts[1]], 1)
    put("put_g", [g_up, low1], [(0, 1, 3), (cuts[1], 3, 2)])
    e_far = two(e_down, -1)
    norm = exchange(norm, 16, 64)
    put("put_e", [e_up, e_down], [(0, 2, 3), (0, 2, 1)])
    serve_norm = in_order(norm)
    put("put_f", [far, g_far], [(0, 0, 2), (0, 1, 2)])
    put("put_h", [e_far, top1], [(0, 2, 2), (0, 3, 2)])
    put("put_last", [low2, top2], [(cuts[2], 3, 2), (cuts[0], 3, 2)])
    return (*outs, serve_norm)


def solution(mesh):
    return jax.shard_map(
        body,
        mesh=mesh,
        in_specs=(
            P("rows", "cols"),
            P("rows", None),
            P(None, "cols"),
            P("rows", "cols"),
            P("rows", None),
            P(None, "cols"),
            P("rows", "cols"),
            P("rows", None),
            P(None, "cols"),
            P(("rows", "cols")),
            P(("rows", "cols")),
        ),
        out_specs=(P("cols", None), P("cols", None), P("cols", None), P()),
        check_vma=False,
    )
```
